512 devices in a mesh: gx: 32 (over x, z), gy: 2 (over y_hi), gz: 8 (over y_lo, core).
Axes of the slice: x: 4, y: 8 (y_hi: 2, y_lo: 4; y = y_hi * 4 + y_lo), z: 8, core: 2. Of those that a mesh axis runs over, the one named last changes fastest.
Arguments:
- coeffs: bfloat16 [16, 1024, 160], P('gz', ('gx', 'gy')), may hold values from -6 to 6
- translations: bfloat16 [16384, 160, 160], P(('gx', 'gz'), 'gy'), may hold values from -0.25 to 0.25
- tmatrix: bfloat16 [1024, 160, 160], P('gx', 'gy'), may hold values from -0.5 to 0.5
- pair_target: int32 [16384], P('gx'), may hold values from 0 to 31
- pair_source: int32 [16384], P('gx'), may hold values from 0 to 1023, as said below
- pair_count: int32 [32], P('gx'), may hold values from 256 to 512, as said below
Outputs:
- result: bfloat16 [16, 1024, 160], P('gz', ('gx', 'gy'))
The draws below stay inside these ranges and needn't reach their ends.
Inputs may be any that keep to these rules, and one draw needn't show every extreme that they name: `pair_count`: some gx group has all 512 slots live in every draw. The source sphere of a slot of group g lies in group g - 1, g or g + 1 modulo 32, that is pair_source[p] // 32 is one of these.
All inputs are finite; a program needn't handle non-finite values.
Results may differ from the reference program's by a relative error of at most 0.009.
Values may be sent and summed in bfloat16 or wider, within the bound.
No kernel may reach another device: no remote copies, remote signals or barrier semaphores. Data moves between devices by JAX's collectives and lax.ppermute only.
A program may use at most 64 MiB of HBM per device.

```python
import jax
import jax.numpy as jnp
from jax import lax

L = 160
R = 16
SPH_X = 32
GROUPS = 32
SPHERES = 1024
PAIR_GRP = 512
PAIRS = 16384


def draw_pair_count(key, part):
    counts = jax.random.randint(key, (GROUPS,), PAIR_GRP // 2, PAIR_GRP + 1)
    fullest = jax.random.randint(jax.random.fold_in(key, 7), (), 0, GROUPS)
    return jnp.where(jnp.arange(GROUPS) == fullest, PAIR_GRP, counts).astype(jnp.int32)


def draw_pair_source(key, part):
    owner = (jnp.arange(PAIRS, dtype=jnp.int32) // PAIR_GRP).astype(jnp.int32)
    offset = jax.random.randint(jax.random.fold_in(key, 11), (PAIRS,), -1, 2)
    within = jax.random.randint(jax.random.fold_in(key, 13), (PAIRS,), 0, SPH_X)
    group = (owner + offset + GROUPS) % GROUPS
    return (group * SPH_X + within).astype(jnp.int32)


def place_ends(drawn, rng, smallest, top_value):
    place = [jax.random.randint(jax.random.fold_in(rng, axis), (), 0, length) for axis, length in enumerate(drawn.shape)]
    longest = drawn.shape.index(max(drawn.shape))
    next_to = place[:longest] + [(place[longest] + 1) % drawn.shape[longest]] + place[longest + 1:]
    return drawn.at[tuple(place)].set(smallest).at[tuple(next_to)].set(top_value)


def block_scale(stream_key, shape, split, least, largest):
    level = 1.0
    for dim, parts in split:
        steps = jax.random.uniform(jax.random.fold_in(jax.random.fold_in(stream_key, 6), dim), (parts,), jnp.float32, least / len(split), largest / len(split))
        level = level * jnp.repeat(jnp.exp(steps), shape[dim] // parts).reshape((-1,) + (1,) * (len(shape) - 1 - dim))
    return level


def gaussian(key, extent, deviation, most, pieces=(), held_as=jnp.bfloat16):
    drawn = deviation * jax.random.normal(key, extent, jnp.float32)
    if pieces:
        drawn = drawn * block_scale(key, extent, pieces, -0.22, 0.18)
    return jnp.clip(drawn, -most, most).astype(held_as)


def setup_inputs(seed: int = 0) -> dict:
    arg_keys = jax.random.split(jax.random.key(seed), 7)
    return {
        "coeffs": gaussian(arg_keys[0], (R, SPHERES, L), 1.0, 6.0, ((0, 8), (1, 64))),
        "translations": gaussian(arg_keys[1], (PAIRS, L, L), (4 * L) ** -0.5, 0.25, ((0, 256), (1, 2))),
        "tmatrix": gaussian(arg_keys[2], (SPHERES, L, L), L ** -0.5, 0.5, ((0, 32), (1, 2))),
        "pair_target": place_ends(jax.random.randint(arg_keys[3], (PAIRS,), 0, SPH_X), jax.random.fold_in(arg_keys[3], 1), 0, SPH_X - 1).astype(jnp.int32),
        "pair_source": draw_pair_source(jax.random.fold_in(arg_keys[6], 71), 0),
        "pair_count": draw_pair_count(jax.random.fold_in(arg_keys[6], 71), 0),
    }


def one_group(coeffs, group_data):
    blocks, target, source, live_count, tmat, own_rows = group_data
    picked = jnp.take(coeffs, source, axis=1).astype(jnp.float32)
    contrib = jnp.einsum('pkl,rpl->rpk', blocks.astype(jnp.float32), picked)
    living = jnp.arange(PAIR_GRP).astype(jnp.int32) < live_count
    spheres_here = jnp.arange(SPH_X).astype(jnp.int32)
    select = ((target[None, :] == spheres_here[:, None]) & living[None, :]).astype(jnp.float32)
    near_field = jnp.einsum('sp,rpk->rsk', select, contrib).astype(jnp.bfloat16)
    scattered = jnp.einsum('rsc,sci->rsi', near_field.astype(jnp.float32), tmat.astype(jnp.float32))
    return (own_rows.astype(jnp.float32) - scattered).astype(jnp.bfloat16)


def reference(coeffs, translations, tmatrix, pair_target, pair_source, pair_count):
    blocks = translations.reshape(GROUPS, PAIR_GRP, L, L)
    targets = pair_target.reshape(GROUPS, PAIR_GRP)
    sources = pair_source.reshape(GROUPS, PAIR_GRP)
    tmats = tmatrix.reshape(GROUPS, SPH_X, L, L)
    own_rows = coeffs.reshape(R, GROUPS, SPH_X, L).transpose(1, 0, 2, 3)
    outputs = lax.map(lambda item: one_group(coeffs, item), (blocks, targets, sources, pair_count, tmats, own_rows))
    return outputs.transpose(1, 0, 2, 3).reshape(R, SPHERES, L)
```

```python
import functools

import jax
import jax.numpy as jnp
from jax import lax
from jax.experimental import pallas as pl
from jax.experimental.pallas import tpu as pltpu
from jax.sharding import PartitionSpec as P

LANES = 128
COLUMN = ("gy", "gz")


def pack_rows(full, rest):
    rows = full.shape[0]
    quarter = rows // 4
    lane = lax.broadcasted_iota(jnp.int32, (quarter, LANES), 1)
    packed = rest[:quarter]
    for q in range(1, 4):
        part = pltpu.roll(rest[q * quarter : (q + 1) * quarter], 32 * q, 1)
        packed = jnp.where(lane < 32 * q, packed, part)
    return jnp.concatenate([full, packed], axis=0)


def unpack_rest(packed):
    parts = [packed] + [pltpu.roll(packed, LANES - 32 * q, 1) for q in range(1, 4)]
    return jnp.concatenate(parts, axis=0)


def widen(value):
    rows = value.shape[0]
    return jnp.concatenate([value, jnp.zeros((rows, LANES - value.shape[1]), value.dtype)], axis=1)


def pack_kernel(x_ref, out_ref):
    rhs, spheres, length = x_ref.shape
    x = x_ref[...].astype(jnp.float32).reshape(rhs * spheres, length)
    packed = pack_rows(x[:, :LANES], widen(x[:, LANES:])).astype(jnp.bfloat16)
    for d in range(out_ref.shape[0]):
        out_ref[d] = packed


def field_kernel(
    target_ref, source_ref, count_ref, own_ref, a_ref, b_ref, trans_ref, tmat_ref, out_ref,
    full_ref, rest_ref, near_ref, sfull_ref, srest_ref,
):
    here = lax.axis_index("gx")
    groups = lax.axis_size("gx")
    base = lax.axis_index("gz") * trans_ref.shape[0]
    spheres = tmat_ref.shape[0]
    half = spheres // 2
    members = own_ref.shape[0]
    rows = own_ref.shape[1] * 4 // 5
    length = trans_ref.shape[2]
    for b, ref in enumerate((own_ref, a_ref, b_ref)):
        for d in range(members):
            piece = ref[d].astype(jnp.float32)
            at = (b * members + d) * rows
            full_ref[at : at + rows, :] = piece[:rows]
            rest_ref[at : at + rows, :] = unpack_rest(piece[rows:])
    near_ref[...] = jnp.zeros_like(near_ref)
    even = lax.rem(here, 2) == 0
    for p in range(trans_ref.shape[0]):
        source = source_ref[base + p]
        group = lax.div(source, spheres)
        sphere = lax.rem(source, spheres)
        relative = lax.rem(group - here + 1 + groups, groups)
        block = jnp.where(relative == 1, 0, jnp.where((relative == 2) == even, 1, 2))
        start = (block * members + lax.div(sphere, half) * (members // 2)) * rows + lax.rem(sphere, half)
        picked = []
        for r in range(2):
            at = pl.ds(start + r * half, members // 2, stride=rows)
            picked.append(
                jnp.concatenate([full_ref[at, :], rest_ref[at, :][:, : length - LANES]], axis=1)
            )
        x = jnp.concatenate(picked, axis=0).astype(jnp.bfloat16)
        contrib = lax.dot_general(
            x, trans_ref[p], (((1,), (1,)), ((), ())), preferred_element_type=jnp.float32
        )
        slot = jnp.where(base + p < count_ref[0], target_ref[base + p], spheres)
        near_ref[slot] = near_ref[slot] + contrib
    for s in range(spheres):
        near = near_ref[s].astype(jnp.bfloat16)
        scattered = jnp.dot(near, tmat_ref[s], preferred_element_type=jnp.float32)
        start = (s // half) * (members // 2) * rows + s % half
        for r in range(2):
            at = pl.ds(start + r * half, members // 2, stride=rows)
            part = scattered[r * (members // 2) : (r + 1) * (members // 2)]
            sfull_ref[at, :] = part[:, :LANES]
            srest_ref[at, :] = widen(part[:, LANES:])
    for d in range(members):
        at = slice(d * rows, (d + 1) * rows)
        out_ref[d] = pack_rows(sfull_ref[at, :], srest_ref[at, :]).astype(jnp.bfloat16)


def final_kernel(x_ref, parts_ref, out_ref):
    rhs, spheres, length = x_ref.shape
    rows = rhs * spheres
    total = parts_ref[0].astype(jnp.float32)
    for d in range(1, parts_ref.shape[0]):
        total = total + parts_ref[d].astype(jnp.float32)
    rest = unpack_rest(total[rows:])[:, : length - LANES]
    scattered = jnp.concatenate([total[:rows], rest], axis=1)
    x = x_ref[...].astype(jnp.float32).reshape(rows, length)
    out_ref[...] = (x - scattered).astype(jnp.bfloat16).reshape(rhs, spheres, length)


def vmem(count):
    return [pl.BlockSpec(memory_space=pltpu.VMEM)] * count


def per_device(coeffs, translations, tmatrix, pair_target, pair_source, pair_count):
    groups = lax.axis_size("gx")
    members = lax.axis_size("gy") * lax.axis_size("gz")
    rhs, spheres, length = coeffs.shape
    rows = rhs * spheres
    packed = rows * length // LANES
    piece = jax.ShapeDtypeStruct((members, packed, LANES), jnp.bfloat16)
    shards = pl.pallas_call(
        pack_kernel, out_shape=piece, in_specs=vmem(1), out_specs=vmem(1)[0], name="pack"
    )(coeffs)
    own = lax.all_to_all(shards, COLUMN, split_axis=0, concat_axis=0, tiled=True)
    pairs_a = [(g, g ^ 1) for g in range(groups)]
    pairs_b = [(g, (g + 1 if g % 2 else g - 1) % groups) for g in range(groups)]
    side_a = lax.ppermute(own, "gx", pairs_a)
    side_b = lax.ppermute(own, "gx", pairs_b)
    smem = pl.BlockSpec(memory_space=pltpu.SMEM)
    window = 3 * members * rows
    parts = pl.pallas_call(
        field_kernel,
        out_shape=piece,
        in_specs=[smem, smem, smem] + vmem(5),
        out_specs=vmem(1)[0],
        scratch_shapes=[
            pltpu.VMEM((window, LANES), jnp.float32),
            pltpu.VMEM((window, LANES), jnp.float32),
            pltpu.VMEM((tmatrix.shape[0] + 1, members, translations.shape[1]), jnp.float32),
            pltpu.VMEM((members * rows, LANES), jnp.float32),
            pltpu.VMEM((members * rows, LANES), jnp.float32),
        ],
        name="field",
    )(pair_target, pair_source, pair_count, own, side_a, side_b, translations, tmatrix)
    arrived = lax.all_to_all(parts, COLUMN, split_axis=0, concat_axis=0, tiled=True)
    return pl.pallas_call(
        final_kernel,
        out_shape=jax.ShapeDtypeStruct(coeffs.shape, coeffs.dtype),
        in_specs=vmem(2),
        out_specs=vmem(1)[0],
        name="final",
    )(coeffs, arrived)


def solution(mesh):
    placed = (
        P("gz", ("gx", "gy"), None),
        P(("gx", "gz"), "gy", None),
        P("gx", "gy", None),
        P("gx"),
        P("gx"),
        P("gx"),
    )
    return jax.shard_map(
        per_device,
        mesh=mesh,
        in_specs=placed,
        out_specs=P("gz", ("gx", "gy"), None),
        check_vma=False,
    )
```

```python
import jax
import jax.numpy as jnp
from jax import lax
from jax.experimental import pallas as pl
from jax.experimental.pallas import tpu as pltpu
from jax.sharding import PartitionSpec as P


LANES = 128
COLUMN = ("gy", "gz")
CHUNKS = 4
VMEM = pl.BlockSpec(memory_space=pltpu.VMEM)
SMEM = pl.BlockSpec(memory_space=pltpu.SMEM)
HBM = pl.BlockSpec(memory_space=pltpu.HBM)


def pack_rows(full, rest):
    quarter = full.shape[0] // 4
    lane = lax.broadcasted_iota(jnp.int32, (quarter, LANES), 1)
    packed = rest[:quarter]
    for q in range(1, 4):
        part = pltpu.roll(rest[q * quarter : (q + 1) * quarter], 32 * q, 1)
        packed = jnp.where(lane < 32 * q, packed, part)
    return jnp.concatenate([full, packed], axis=0)


def unpack_rest(packed):
    parts = [packed] + [pltpu.roll(packed, LANES - 32 * q, 1) for q in range(1, 4)]
    return jnp.concatenate(parts, axis=0)


def widen(value):
    rows = value.shape[0]
    return jnp.concatenate([value, jnp.zeros((rows, LANES - value.shape[1]), value.dtype)], axis=1)


def pack_kernel(x_ref, out_ref):
    rhs, spheres, length = x_ref.shape
    x = x_ref[...].astype(jnp.float32).reshape(rhs * spheres, length)
    packed = pack_rows(x[:, :LANES], widen(x[:, LANES:])).astype(jnp.bfloat16)
    for d in range(out_ref.shape[0]):
        out_ref[d] = packed


def field_kernel(
    start_ref, slot_ref, left_ref, own_ref, right_ref, trans_hbm, tmat_hbm, out_ref,
    trans_ref, tmat_ref, full_ref, rest_ref, near_ref, sfull_ref, srest_ref, sems,
):
    slots = trans_ref.shape[0]
    spheres = tmat_ref.shape[0]
    part = slots // CHUNKS
    copies = [
        pltpu.make_async_copy(
            trans_hbm.at[pl.ds(c * part, part)], trans_ref.at[pl.ds(c * part, part)], sems.at[c]
        )
        for c in range(CHUNKS)
    ]
    copies.append(pltpu.make_async_copy(tmat_hbm, tmat_ref, sems.at[CHUNKS]))
    for copy in copies:
        copy.start()
    half = spheres // 2
    length = trans_ref.shape[2]
    members = near_ref.shape[1]
    rows = full_ref.shape[0] // (3 * members)

    def place(piece, at):
        piece = piece.astype(jnp.float32)
        full_ref[pl.ds(at, rows), :] = piece[:rows]
        rest_ref[pl.ds(at, rows), :] = unpack_rest(piece[rows:])

    for b, ref in enumerate((left_ref, own_ref, right_ref)):
        for d in range(members):
            place(ref[d], (b * members + d) * rows)
    near_ref[...] = jnp.zeros_like(near_ref)
    for p in range(slots):
        if p % part == 0:
            copies[p // part].wait()
        start = start_ref[p]
        picked = []
        for r in range(2):
            at = pl.ds(start + r * half, members // 2, stride=rows)
            picked.append(
                jnp.concatenate([full_ref[at, :], rest_ref[at, :][:, : length - LANES]], axis=1)
            )
        x = jnp.concatenate(picked, axis=0).astype(jnp.bfloat16)
        contrib = lax.dot_general(
            x, trans_ref[p], (((1,), (1,)), ((), ())), preferred_element_type=jnp.float32
        )
        slot = slot_ref[p]
        near_ref[slot] = near_ref[slot] + contrib
    copies[CHUNKS].wait()
    for s in range(spheres):
        near = near_ref[s].astype(jnp.bfloat16)
        scattered = jnp.dot(near, tmat_ref[s], preferred_element_type=jnp.float32)
        start = (s // half) * (members // 2) * rows + s % half
        for r in range(2):
            at = pl.ds(start + r * half, members // 2, stride=rows)
            value = scattered[r * (members // 2) : (r + 1) * (members // 2)]
            sfull_ref[at, :] = value[:, :LANES]
            srest_ref[at, :] = widen(value[:, LANES:])
    for d in range(members):
        at = slice(d * rows, (d + 1) * rows)
        out_ref[d] = pack_rows(sfull_ref[at, :], srest_ref[at, :]).astype(jnp.bfloat16)


def final_kernel(x_ref, parts_ref, out_ref):
    rhs, spheres, length = x_ref.shape
    rows = rhs * spheres
    total = parts_ref[0].astype(jnp.float32)
    for d in range(1, parts_ref.shape[0]):
        total = total + parts_ref[d].astype(jnp.float32)
    rest = unpack_rest(total[rows:])[:, : length - LANES]
    scattered = jnp.concatenate([total[:rows], rest], axis=1)
    x = x_ref[...].astype(jnp.float32).reshape(rows, length)
    out_ref[...] = (x - scattered).astype(jnp.bfloat16).reshape(rhs, spheres, length)


def limit(mebibytes):
    return pltpu.CompilerParams(vmem_limit_bytes=mebibytes * 2**20)


def bf16(*shape):
    return jax.ShapeDtypeStruct(shape, jnp.bfloat16)


def per_device(coeffs, translations, tmatrix, pair_target, pair_source, pair_count):
    groups = lax.axis_size("gx")
    members = lax.axis_size("gy") * lax.axis_size("gz")
    rhs, spheres, length = coeffs.shape
    rows = rhs * spheres
    packed = rows * length // LANES
    up = [(g, (g + 1) % groups) for g in range(groups)]
    down = [(g, (g - 1) % groups) for g in range(groups)]
    shards = pl.pallas_call(
        pack_kernel, out_shape=bf16(members, packed, LANES), in_specs=[VMEM], out_specs=VMEM,
        compiler_params=limit(2), name="pack",
    )(coeffs)
    own = lax.all_to_all(shards, COLUMN, split_axis=0, concat_axis=0, tiled=True)
    left = lax.ppermute(own, "gx", up)
    right = lax.ppermute(own, "gx", down)
    window = (left, own, right)
    rows_window = 3 * members * rows
    slots = translations.shape[0]
    group_spheres = tmatrix.shape[0]
    base = lax.axis_index("gz") * slots
    source = lax.dynamic_slice_in_dim(pair_source, base, slots)
    target = lax.dynamic_slice_in_dim(pair_target, base, slots)
    relative = (source // group_spheres - lax.axis_index("gx") + 1 + groups) % groups
    sphere = source % group_spheres
    holder = (relative * 2 + sphere // spheres) * (members // 2)
    start = holder * rows + sphere % spheres
    living = base + jnp.arange(slots, dtype=jnp.int32) < pair_count[0]
    slot = jnp.where(living, target, group_spheres)
    parts = pl.pallas_call(
        field_kernel,
        out_shape=bf16(members, packed, LANES),
        in_specs=[SMEM] * 2 + [VMEM] * len(window) + [HBM] * 2,
        out_specs=VMEM,
        scratch_shapes=[
            pltpu.VMEM(translations.shape, jnp.bfloat16),
            pltpu.VMEM(tmatrix.shape, jnp.bfloat16),
            pltpu.VMEM((rows_window, LANES), jnp.float32),
            pltpu.VMEM((rows_window, LANES), jnp.float32),
            pltpu.VMEM((tmatrix.shape[0] + 1, members, translations.shape[1]), jnp.float32),
            pltpu.VMEM((members * rows, LANES), jnp.float32),
            pltpu.VMEM((members * rows, LANES), jnp.float32),
            pltpu.SemaphoreType.DMA((CHUNKS + 1,)),
        ],
        compiler_params=limit(53),
        name="field",
    )(start, slot, *window, translations, tmatrix)
    arrived = lax.all_to_all(parts, COLUMN, split_axis=0, concat_axis=0, tiled=True)
    return pl.pallas_call(
        final_kernel, out_shape=bf16(*coeffs.shape), in_specs=[VMEM] * 2, out_specs=VMEM,
        compiler_params=limit(2), name="final",
    )(coeffs, arrived)


def solution(mesh):
    placed = (
        P("gz", ("gx", "gy"), None),
        P(("gx", "gz"), "gy", None),
        P("gx", "gy", None),
        P("gx"),
        P("gx"),
        P("gx"),
    )
    return jax.shard_map(
        per_device,
        mesh=mesh,
        in_specs=placed,
        out_specs=P("gz", ("gx", "gy"), None),
        check_vma=False,
    )
```

```python
import jax
import jax.numpy as jnp
from jax import lax
from jax.experimental import pallas as pl
from jax.experimental.pallas import tpu as pltpu
from jax.sharding import PartitionSpec as P


LANES = 128
COLUMN = ("gy", "gz")
CHUNKS = 4
VMEM = pl.BlockSpec(memory_space=pltpu.VMEM)
HBM = pl.BlockSpec(memory_space=pltpu.HBM)


def pack_rows(full, rest):
    quarter = full.shape[0] // 4
    lane = lax.broadcasted_iota(jnp.int32, (quarter, LANES), 1)
    packed = rest[:quarter]
    for q in range(1, 4):
        part = pltpu.roll(rest[q * quarter : (q + 1) * quarter], 32 * q, 1)
        packed = jnp.where(lane < 32 * q, packed, part)
    return jnp.concatenate([full, packed], axis=0)


def unpack_rest(packed):
    parts = [packed] + [pltpu.roll(packed, LANES - 32 * q, 1) for q in range(1, 4)]
    return jnp.concatenate(parts, axis=0)


def widen(value):
    rows = value.shape[0]
    return jnp.concatenate([value, jnp.zeros((rows, LANES - value.shape[1]), value.dtype)], axis=1)


def pack_kernel(x_ref, out_ref):
    rhs, spheres, length = x_ref.shape
    x = x_ref[...].astype(jnp.float32).reshape(rhs * spheres, length)
    packed = pack_rows(x[:, :LANES], widen(x[:, LANES:])).astype(jnp.bfloat16)
    for d in range(out_ref.shape[0]):
        out_ref[d] = packed


def contract_kernel(
    table_hbm, left_ref, own_ref, right_ref, mine_ref, other_hbm, near_out,
    table_ref, other_ref, full_ref, rest_ref, near_ref, sems,
):
    table_copy = pltpu.make_async_copy(table_hbm, table_ref, sems.at[0])
    table_copy.start()
    part = other_ref.shape[0] // CHUNKS
    copies = []
    for c in range(CHUNKS):
        at = pl.ds(c * part, part)
        copies.append(pltpu.make_async_copy(other_hbm.at[at], other_ref.at[at], sems.at[c + 1]))
        copies[c].start()
    slots = mine_ref.shape[0]
    spheres, rhs, _ = near_out.shape
    length = mine_ref.shape[2]
    members = own_ref.shape[0]
    rows = own_ref.shape[1] * LANES // length
    core = lax.rem(lax.axis_index("gz"), 2)
    for b, ref in enumerate((left_ref, own_ref, right_ref)):
        for d in range(members):
            at = (b * members + d) * rows
            piece = ref[d].astype(jnp.float32)
            full_ref[at : at + rows, :] = piece[:rows]
            rest_ref[at : at + rows, :] = unpack_rest(piece[rows:])
    near_ref[...] = jnp.zeros_like(near_ref)
    table_copy.wait()
    for ref, base in ((mine_ref, core * slots), (other_ref, (1 - core) * slots)):
        for p in range(slots):
            if ref is other_ref and p % part == 0:
                copies[p // part].wait()
            at = pl.ds(table_ref[0, base + p], rhs, stride=spheres // 2)
            x = jnp.concatenate([full_ref[at, :], rest_ref[at, :][:, : length - LANES]], axis=1)
            contrib = lax.dot_general(
                x.astype(jnp.bfloat16), ref[p], (((1,), (1,)), ((), ())),
                preferred_element_type=jnp.float32,
            )
            slot = table_ref[1, base + p]
            near_ref[slot] = near_ref[slot] + contrib
    near_out[...] = near_ref[:spheres].astype(jnp.bfloat16)


def apply_kernel(near_ref, tmat_ref, out_ref, full_ref, rest_ref):
    spheres, rhs, _ = near_ref.shape
    half = spheres // 2
    members = out_ref.shape[0]
    rows = full_ref.shape[0] // members
    for s in range(spheres):
        scattered = jnp.dot(near_ref[s], tmat_ref[s], preferred_element_type=jnp.float32)
        at = pl.ds((s // half) * rhs * half + s % half, rhs, stride=half)
        full_ref[at, :] = scattered[:, :LANES]
        rest_ref[at, :] = widen(scattered[:, LANES:])
    for d in range(members):
        at = slice(d * rows, (d + 1) * rows)
        out_ref[d] = pack_rows(full_ref[at, :], rest_ref[at, :]).astype(jnp.bfloat16)


def final_kernel(x_ref, parts_ref, out_ref):
    rhs, spheres, length = x_ref.shape
    rows = rhs * spheres
    total = parts_ref[0].astype(jnp.float32)
    for d in range(1, parts_ref.shape[0]):
        total = total + parts_ref[d].astype(jnp.float32)
    rest = unpack_rest(total[rows:])[:, : length - LANES]
    scattered = jnp.concatenate([total[:rows], rest], axis=1)
    x = x_ref[...].astype(jnp.float32).reshape(rows, length)
    out_ref[...] = (x - scattered).astype(jnp.bfloat16).reshape(rhs, spheres, length)


def limit(mebibytes):
    return pltpu.CompilerParams(vmem_limit_bytes=mebibytes * 2**20)


def cost(flops, size):
    return pl.CostEstimate(flops=flops, bytes_accessed=size, transcendentals=0)


def bf16(*shape):
    return jax.ShapeDtypeStruct(shape, jnp.bfloat16)


def per_device(coeffs, translations, tmatrix, pair_target, pair_source, pair_count):
    groups = lax.axis_size("gx")
    cores = 2
    members = lax.axis_size("gy") * lax.axis_size("gz") // cores
    rhs, spheres, length = coeffs.shape
    rows = rhs * spheres
    packed = rows * length // LANES
    slots, half_length, _ = translations.shape
    group_spheres = tmatrix.shape[0]
    rhs_core = rhs * lax.axis_size("gz") // cores
    up = [(g, (g + 1) % groups) for g in range(groups)]
    down = [(g, (g - 1) % groups) for g in range(groups)]
    sibling = [(i, i ^ 1) for i in range(lax.axis_size("gz"))]
    same_core = [[cores * y + c for y in range(members)] for c in range(cores)]

    def exchange(pieces):
        return lax.all_to_all(
            pieces, COLUMN, split_axis=0, concat_axis=0, tiled=True, axis_index_groups=same_core
        )

    shards = pl.pallas_call(
        pack_kernel, out_shape=bf16(members, packed, LANES), in_specs=[VMEM], out_specs=VMEM,
        compiler_params=limit(2), cost_estimate=cost(10**9, 2**18), name="pack",
    )(coeffs)
    other = lax.ppermute(translations, "gz", sibling)
    own = exchange(shards)
    left = lax.ppermute(own, "gx", up)
    right = lax.ppermute(own, "gx", down)
    base = lax.axis_index("gz") // cores * (cores * slots)
    source = lax.dynamic_slice_in_dim(pair_source, base, cores * slots)
    target = lax.dynamic_slice_in_dim(pair_target, base, cores * slots)
    relative = (source // group_spheres - lax.axis_index("gx") + 1 + groups) % groups
    sphere = source % group_spheres
    start = (relative * 2 + sphere // spheres) * (rhs_core * spheres) + sphere % spheres
    living = base + jnp.arange(cores * slots, dtype=jnp.int32) < pair_count[0]
    slot = jnp.where(living, target, group_spheres)
    window = pltpu.VMEM((3 * members * rows, LANES), jnp.float32)
    near = pl.pallas_call(
        contract_kernel,
        out_shape=bf16(group_spheres, rhs_core, half_length),
        in_specs=[HBM] + [VMEM] * 4 + [HBM],
        out_specs=VMEM,
        scratch_shapes=[
            pltpu.SMEM((2, cores * slots), jnp.int32),
            pltpu.VMEM(translations.shape, jnp.bfloat16),
            window,
            window,
            pltpu.VMEM((group_spheres + 1, rhs_core, half_length), jnp.float32),
            pltpu.SemaphoreType.DMA((CHUNKS + 1,)),
        ],
        compiler_params=limit(10),
        cost_estimate=cost(4 * rhs_core * translations.size, 4 * translations.size),
        name="contract",
    )(jnp.stack([start, slot]), left, own, right, translations, other)
    parts = pl.pallas_call(
        apply_kernel,
        out_shape=bf16(members, packed, LANES),
        in_specs=[VMEM] * 2,
        out_specs=VMEM,
        scratch_shapes=[pltpu.VMEM((members * rows, LANES), jnp.float32)] * 2,
        compiler_params=limit(4),
        cost_estimate=cost(2 * rhs_core * tmatrix.size, 2 * tmatrix.size),
        name="apply",
    )(near, tmatrix)
    arrived = exchange(parts)
    return pl.pallas_call(
        final_kernel, out_shape=bf16(*coeffs.shape), in_specs=[VMEM] * 2, out_specs=VMEM,
        compiler_params=limit(2), name="final",
    )(coeffs, arrived)


def solution(mesh):
    placed = (
        P("gz", ("gx", "gy"), None),
        P(("gx", "gz"), "gy", None),
        P("gx", "gy", None),
        P("gx"),
        P("gx"),
        P("gx"),
    )
    return jax.shard_map(
        per_device,
        mesh=mesh,
        in_specs=placed,
        out_specs=P("gz", ("gx", "gy"), None),
        check_vma=False,
    )
```

```python
import jax
import jax.numpy as jnp
from jax import lax
from jax.experimental import pallas as pl
from jax.experimental.pallas import tpu as pltpu
from jax.sharding import PartitionSpec as P


LANES = 128
RUN = 8
COLUMN = ("gy", "gz")
VMEM = pl.BlockSpec(memory_space=pltpu.VMEM)
HBM = pl.BlockSpec(memory_space=pltpu.HBM)
SMEM = pl.BlockSpec(memory_space=pltpu.SMEM)


def pack_rows(full, rest):
    quarter = full.shape[0] // 4
    lane = lax.broadcasted_iota(jnp.int32, (quarter, LANES), 1)
    packed = rest[:quarter]
    for q in range(1, 4):
        part = pltpu.roll(rest[q * quarter : (q + 1) * quarter], 32 * q, 1)
        packed = jnp.where(lane < 32 * q, packed, part)
    return jnp.concatenate([full, packed], axis=0)


def unpack_rest(packed):
    parts = [packed] + [pltpu.roll(packed, LANES - 32 * q, 1) for q in range(1, 4)]
    return jnp.concatenate(parts, axis=0)


def widen(value):
    rows = value.shape[0]
    return jnp.concatenate([value, jnp.zeros((rows, LANES - value.shape[1]), value.dtype)], axis=1)


def pack_kernel(count_ref, x_ref, out_ref):
    del count_ref
    rhs, spheres, length = x_ref.shape
    x = x_ref[...].astype(jnp.float32).reshape(rhs * spheres, length)
    packed = pack_rows(x[:, :LANES], widen(x[:, LANES:])).astype(jnp.bfloat16)
    for d in range(out_ref.shape[0]):
        out_ref[d] = packed


def contract_kernel(
    count_ref, source_hbm, target_hbm, own_ref, odd_ref, even_ref, even_last_ref, mine_ref, other_ref, near_out,
    source_ref, target_ref, full_ref, rest_ref, near_ref, sems,
):
    here = lax.axis_index("gx")
    groups = lax.axis_size("gx")
    core = lax.rem(lax.axis_index("gz"), 2)
    base = pl.multiple_of((lax.axis_index("gz") - core) * mine_ref.shape[0], LANES)
    tables = []
    for i, (hbm, ref) in enumerate(((source_hbm, source_ref), (target_hbm, target_ref))):
        tables.append(pltpu.make_async_copy(hbm.at[pl.ds(base, ref.shape[0])], ref, sems.at[i]))
        tables[i].start()
    slots = mine_ref.shape[0]
    spheres, rhs, _ = near_out.shape
    length = mine_ref.shape[2]
    members = own_ref.shape[0]
    rows = own_ref.shape[1] * LANES // length
    odd_block = 2 * lax.rem(here, 2)
    for ref, block in ((own_ref, 1), (odd_ref, odd_block), (even_ref, 2 - odd_block)):
        for d in range(members):
            at = pl.ds(pl.multiple_of((block * members + d) * rows, rows), rows)
            piece = ref[d].astype(jnp.float32)
            if ref is even_ref:
                piece = piece + even_last_ref[d].astype(jnp.float32)
            full_ref[at, :] = piece[:rows]
            rest_ref[at, :] = unpack_rest(piece[rows:])
    near_ref[...] = jnp.zeros_like(near_ref)
    for copy in tables:
        copy.wait()
    half = spheres // 2
    assert half & (half - 1) == 0 and groups & (groups - 1) == 0
    shift = half.bit_length() - 1
    offset = (1 - here + groups) * spheres
    live = count_ref[0] - base
    for ref, first in ((mine_ref, core * slots), (other_ref, (1 - core) * slots)):
        for p in range(slots):
            near_by = (source_ref[first + p] + offset) & (groups * spheres - 1)
            start = lax.shift_right_logical(near_by, shift) * (rhs * half) + (near_by & (half - 1))
            at = pl.ds(start, rhs, stride=half)
            x = jnp.concatenate([full_ref[at, :], rest_ref[at, :][:, : length - LANES]], axis=1)
            contrib = lax.dot_general(
                x.astype(jnp.bfloat16), ref[p], (((1,), (1,)), ((), ())),
                preferred_element_type=jnp.float32,
            )
            slot = jnp.where(first + p < live, target_ref[first + p], spheres)
            near_ref[slot] = near_ref[slot] + contrib
    near_out[...] = near_ref[:spheres].astype(jnp.bfloat16)


def apply_kernel(near_ref, tmat_ref, out_ref, full_ref, rest_ref):
    spheres, rhs, _ = near_ref.shape
    half = spheres // 2
    members = out_ref.shape[0]
    rows = full_ref.shape[0] // members
    for s in range(spheres):
        scattered = jnp.dot(near_ref[s], tmat_ref[s], preferred_element_type=jnp.float32)
        at = pl.ds((s // half) * rhs * half + s % half, rhs, stride=half)
        full_ref[at, :] = scattered[:, :LANES]
        rest_ref[at, :] = widen(scattered[:, LANES:])
    for d in range(members):
        at = slice(d * rows, (d + 1) * rows)
        out_ref[d] = pack_rows(full_ref[at, :], rest_ref[at, :]).astype(jnp.bfloat16)


def final_kernel(x_ref, parts_ref, out_ref):
    rhs, spheres, length = x_ref.shape
    rows = rhs * spheres
    total = parts_ref[0].astype(jnp.float32)
    for d in range(1, parts_ref.shape[0]):
        total = total + parts_ref[d].astype(jnp.float32)
    rest = unpack_rest(total[rows:])[:, : length - LANES]
    scattered = jnp.concatenate([total[:rows], rest], axis=1)
    x = x_ref[...].astype(jnp.float32).reshape(rows, length)
    out_ref[...] = (x - scattered).astype(jnp.bfloat16).reshape(rhs, spheres, length)


def limit(mebibytes):
    return pltpu.CompilerParams(vmem_limit_bytes=mebibytes * 2**20)


def cost(flops, size):
    return pl.CostEstimate(flops=flops, bytes_accessed=size, transcendentals=0)


def bf16(*shape):
    return jax.ShapeDtypeStruct(shape, jnp.bfloat16)


def per_device(coeffs, translations, tmatrix, pair_target, pair_source, pair_count):
    groups = lax.axis_size("gx")
    cores = 2
    members = lax.axis_size("gy") * lax.axis_size("gz") // cores
    rhs, spheres, length = coeffs.shape
    rows = rhs * spheres
    packed = rows * length // LANES
    slots, half_length, _ = translations.shape
    group_spheres = tmatrix.shape[0]
    rhs_core = rhs * lax.axis_size("gz") // cores
    even_pairs = [(g, g ^ 1) for g in range(groups)]
    odd_pairs = [(g, (g + 1 if g % 2 else g - 1) % groups) for g in range(groups)]
    sibling = [(i, i ^ 1) for i in range(lax.axis_size("gz"))]
    same_core = [[cores * y + c for y in range(members)] for c in range(cores)]

    def exchange(pieces):
        return lax.all_to_all(
            pieces, COLUMN, split_axis=0, concat_axis=0, tiled=True, axis_index_groups=same_core
        )

    shards = pl.pallas_call(
        pack_kernel, out_shape=bf16(members, packed, LANES), in_specs=[SMEM, VMEM], out_specs=VMEM,
        compiler_params=limit(2), cost_estimate=cost(10**9, 2**18), name="pack",
    )(pair_count, coeffs)
    other = lax.ppermute(translations, "gz", sibling)
    own = exchange(shards)
    even_first = lax.ppermute(own, "gx", [p for p in even_pairs if p[0] % RUN < RUN - 2])
    odd = lax.ppermute(own, "gx", odd_pairs)
    even_last = lax.ppermute(own, "gx", [p for p in even_pairs if p[0] % RUN >= RUN - 2])
    window = pltpu.VMEM((3 * members * rows, LANES), jnp.float32)
    near = pl.pallas_call(
        contract_kernel,
        out_shape=bf16(group_spheres, rhs_core, half_length),
        in_specs=[SMEM] + [HBM] * 2 + [VMEM] * 6,
        out_specs=VMEM,
        scratch_shapes=[
            pltpu.SMEM((cores * slots,), jnp.int32),
            pltpu.SMEM((cores * slots,), jnp.int32),
            window,
            window,
            pltpu.VMEM((group_spheres + 1, rhs_core, half_length), jnp.float32),
            pltpu.SemaphoreType.DMA((2,)),
        ],
        compiler_params=limit(10),
        cost_estimate=cost(4 * rhs_core * translations.size, 4 * translations.size),
        name="contract",
    )(pair_count, pair_source, pair_target, own, odd, even_first, even_last, translations, other)
    parts = pl.pallas_call(
        apply_kernel,
        out_shape=bf16(members, packed, LANES),
        in_specs=[VMEM] * 2,
        out_specs=VMEM,
        scratch_shapes=[pltpu.VMEM((members * rows, LANES), jnp.float32)] * 2,
        compiler_params=limit(4),
        cost_estimate=cost(2 * rhs_core * tmatrix.size, 2 * tmatrix.size),
        name="apply",
    )(near, tmatrix)
    arrived = exchange(parts)
    return pl.pallas_call(
        final_kernel, out_shape=bf16(*coeffs.shape), in_specs=[VMEM] * 2, out_specs=VMEM,
        compiler_params=limit(2), name="final",
    )(coeffs, arrived)


def solution(mesh):
    placed = (
        P("gz", ("gx", "gy"), None),
        P(("gx", "gz"), "gy", None),
        P("gx", "gy", None),
        P("gx"),
        P("gx"),
        P("gx"),
    )
    return jax.shard_map(
        per_device,
        mesh=mesh,
        in_specs=placed,
        out_specs=P("gz", ("gx", "gy"), None),
        check_vma=False,
    )
```

```python
import jax
import jax.numpy as jnp
from jax import lax
from jax.experimental import pallas as pl
from jax.experimental.pallas import tpu as pltpu
from jax.sharding import PartitionSpec as P


LANES = 128
CHUNKS = 2
RUN = 8
COLUMN = ("gy", "gz")
VMEM = pl.BlockSpec(memory_space=pltpu.VMEM)
HBM = pl.BlockSpec(memory_space=pltpu.HBM)
SMEM = pl.BlockSpec(memory_space=pltpu.SMEM)


def pack_rows(full, rest):
    quarter = full.shape[0] // 4
    lane = lax.broadcasted_iota(jnp.int32, (quarter, LANES), 1)
    packed = rest[:quarter]
    for q in range(1, 4):
        part = pltpu.roll(rest[q * quarter : (q + 1) * quarter], 32 * q, 1)
        packed = jnp.where(lane < 32 * q, packed, part)
    return jnp.concatenate([full, packed], axis=0)


def unpack_rest(packed):
    parts = [packed] + [pltpu.roll(packed, LANES - 32 * q, 1) for q in range(1, 4)]
    return jnp.concatenate(parts, axis=0)


def widen(value):
    rows = value.shape[0]
    return jnp.concatenate([value, jnp.zeros((rows, LANES - value.shape[1]), value.dtype)], axis=1)


def pack_kernel(x_ref, out_ref):
    rhs, spheres, length = x_ref.shape
    x = x_ref[...].astype(jnp.float32).reshape(rhs * spheres, length)
    packed = pack_rows(x[:, :LANES], widen(x[:, LANES:])).astype(jnp.bfloat16)
    for d in range(out_ref.shape[0]):
        out_ref[d] = packed


def contract_kernel(
    count_ref, source_hbm, target_hbm, own_ref, odd_ref, even_ref, even_last_ref, mine_ref, other_hbm, near_out,
    source_ref, target_ref, other_ref, full_ref, rest_ref, near_ref, sems,
):
    here = lax.axis_index("gx")
    groups = lax.axis_size("gx")
    core = lax.rem(lax.axis_index("gz"), 2)
    base = pl.multiple_of((lax.axis_index("gz") - core) * mine_ref.shape[0], LANES)
    tables = []
    for i, (hbm, ref) in enumerate(((source_hbm, source_ref), (target_hbm, target_ref))):
        tables.append(pltpu.make_async_copy(hbm.at[pl.ds(base, ref.shape[0])], ref, sems.at[i]))
        tables[i].start()
    part = other_ref.shape[0] // CHUNKS
    copies = []
    for c in range(CHUNKS):
        at = pl.ds(c * part, part)
        copies.append(pltpu.make_async_copy(other_hbm.at[at], other_ref.at[at], sems.at[c + 2]))
        copies[c].start()
    slots = mine_ref.shape[0]
    spheres, rhs, _ = near_out.shape
    length = mine_ref.shape[2]
    members = own_ref.shape[0]
    rows = own_ref.shape[1] * LANES // length
    odd_block = 2 * lax.rem(here, 2)
    for ref, block in ((own_ref, 1), (odd_ref, odd_block), (even_ref, 2 - odd_block)):
        for d in range(members):
            at = pl.ds(pl.multiple_of((block * members + d) * rows, rows), rows)
            piece = ref[d].astype(jnp.float32)
            if ref is even_ref:
                piece = piece + even_last_ref[d].astype(jnp.float32)
            full_ref[at, :] = piece[:rows]
            rest_ref[at, :] = unpack_rest(piece[rows:])
    near_ref[...] = jnp.zeros_like(near_ref)
    for copy in tables:
        copy.wait()
    half = spheres // 2
    assert half & (half - 1) == 0 and groups & (groups - 1) == 0
    shift = half.bit_length() - 1
    offset = (1 - here + groups) * spheres
    live = count_ref[0] - base
    for ref, first in ((mine_ref, core * slots), (other_ref, (1 - core) * slots)):
        for p in range(slots):
            if ref is other_ref and p % part == 0:
                copies[p // part].wait()
            near_by = (source_ref[first + p] + offset) & (groups * spheres - 1)
            start = lax.shift_right_logical(near_by, shift) * (rhs * half) + (near_by & (half - 1))
            at = pl.ds(start, rhs, stride=half)
            x = jnp.concatenate([full_ref[at, :], rest_ref[at, :][:, : length - LANES]], axis=1)
            contrib = lax.dot_general(
                x.astype(jnp.bfloat16), ref[p], (((1,), (1,)), ((), ())),
                preferred_element_type=jnp.float32,
            )
            slot = jnp.where(first + p < live, target_ref[first + p], spheres)
            near_ref[slot] = near_ref[slot] + contrib
    near_out[...] = near_ref[:spheres].astype(jnp.bfloat16)


def apply_kernel(near_ref, tmat_ref, out_ref, full_ref, rest_ref):
    spheres, rhs, _ = near_ref.shape
    half = spheres // 2
    members = out_ref.shape[0]
    rows = full_ref.shape[0] // members
    for s in range(spheres):
        scattered = jnp.dot(near_ref[s], tmat_ref[s], preferred_element_type=jnp.float32)
        at = pl.ds((s // half) * rhs * half + s % half, rhs, stride=half)
        full_ref[at, :] = scattered[:, :LANES]
        rest_ref[at, :] = widen(scattered[:, LANES:])
    for d in range(members):
        at = slice(d * rows, (d + 1) * rows)
        out_ref[d] = pack_rows(full_ref[at, :], rest_ref[at, :]).astype(jnp.bfloat16)


def final_kernel(x_ref, parts_ref, out_ref):
    rhs, spheres, length = x_ref.shape
    rows = rhs * spheres
    total = parts_ref[0].astype(jnp.float32)
    for d in range(1, parts_ref.shape[0]):
        total = total + parts_ref[d].astype(jnp.float32)
    rest = unpack_rest(total[rows:])[:, : length - LANES]
    scattered = jnp.concatenate([total[:rows], rest], axis=1)
    x = x_ref[...].astype(jnp.float32).reshape(rows, length)
    out_ref[...] = (x - scattered).astype(jnp.bfloat16).reshape(rhs, spheres, length)


def limit(mebibytes):
    return pltpu.CompilerParams(vmem_limit_bytes=mebibytes * 2**20)


def cost(flops, size):
    return pl.CostEstimate(flops=flops, bytes_accessed=size, transcendentals=0)


def bf16(*shape):
    return jax.ShapeDtypeStruct(shape, jnp.bfloat16)


def per_device(coeffs, translations, tmatrix, pair_target, pair_source, pair_count):
    groups = lax.axis_size("gx")
    cores = 2
    members = lax.axis_size("gy") * lax.axis_size("gz") // cores
    rhs, spheres, length = coeffs.shape
    rows = rhs * spheres
    packed = rows * length // LANES
    slots, half_length, _ = translations.shape
    group_spheres = tmatrix.shape[0]
    rhs_core = rhs * lax.axis_size("gz") // cores
    even_pairs = [(g, g ^ 1) for g in range(groups)]
    odd_pairs = [(g, (g + 1 if g % 2 else g - 1) % groups) for g in range(groups)]
    sibling = [(i, i ^ 1) for i in range(lax.axis_size("gz"))]
    same_core = [[cores * y + c for y in range(members)] for c in range(cores)]

    def exchange(pieces):
        return lax.all_to_all(
            pieces, COLUMN, split_axis=0, concat_axis=0, tiled=True, axis_index_groups=same_core
        )

    shards = pl.pallas_call(
        pack_kernel, out_shape=bf16(members, packed, LANES), in_specs=[VMEM], out_specs=VMEM,
        compiler_params=limit(2), cost_estimate=cost(10**9, 2**18), name="pack",
    )(coeffs)
    other = lax.ppermute(translations, "gz", sibling)
    own = exchange(shards)
    even_first = lax.ppermute(own, "gx", [p for p in even_pairs if p[0] % RUN < RUN - 2])
    odd = lax.ppermute(own, "gx", odd_pairs)
    even_last = lax.ppermute(own, "gx", [p for p in even_pairs if p[0] % RUN >= RUN - 2])
    window = pltpu.VMEM((3 * members * rows, LANES), jnp.float32)
    near = pl.pallas_call(
        contract_kernel,
        out_shape=bf16(group_spheres, rhs_core, half_length),
        in_specs=[SMEM] + [HBM] * 2 + [VMEM] * 5 + [HBM],
        out_specs=VMEM,
        scratch_shapes=[
            pltpu.SMEM((cores * slots,), jnp.int32),
            pltpu.SMEM((cores * slots,), jnp.int32),
            pltpu.VMEM(translations.shape, jnp.bfloat16),
            window,
            window,
            pltpu.VMEM((group_spheres + 1, rhs_core, half_length), jnp.float32),
            pltpu.SemaphoreType.DMA((CHUNKS + 2,)),
        ],
        compiler_params=limit(10),
        cost_estimate=cost(4 * rhs_core * translations.size, 4 * translations.size),
        name="contract",
    )(pair_count, pair_source, pair_target, own, odd, even_first, even_last, translations, other)
    parts = pl.pallas_call(
        apply_kernel,
        out_shape=bf16(members, packed, LANES),
        in_specs=[VMEM] * 2,
        out_specs=VMEM,
        scratch_shapes=[pltpu.VMEM((members * rows, LANES), jnp.float32)] * 2,
        compiler_params=limit(4),
        cost_estimate=cost(2 * rhs_core * tmatrix.size, 2 * tmatrix.size),
        name="apply",
    )(near, tmatrix)
    arrived = exchange(parts)
    return pl.pallas_call(
        final_kernel, out_shape=bf16(*coeffs.shape), in_specs=[VMEM] * 2, out_specs=VMEM,
        compiler_params=limit(2), name="final",
    )(coeffs, arrived)


def solution(mesh):
    placed = (
        P("gz", ("gx", "gy"), None),
        P(("gx", "gz"), "gy", None),
        P("gx", "gy", None),
        P("gx"),
        P("gx"),
        P("gx"),
    )
    return jax.shard_map(
        per_device,
        mesh=mesh,
        in_specs=placed,
        out_specs=P("gz", ("gx", "gy"), None),
        check_vma=False,
    )
```

```python
import jax
import jax.numpy as jnp
from jax import lax
from jax.experimental import pallas as pl
from jax.experimental.pallas import tpu as pltpu
from jax.sharding import PartitionSpec as P


LANES = 128
CHUNKS = 2
RUN = 8
COLUMN = ("gy", "gz")
VMEM = pl.BlockSpec(memory_space=pltpu.VMEM)
HBM = pl.BlockSpec(memory_space=pltpu.HBM)
SMEM = pl.BlockSpec(memory_space=pltpu.SMEM)


def pack_rows(full, rest):
    quarter = full.shape[0] // 4
    lane = lax.broadcasted_iota(jnp.int32, (quarter, LANES), 1)
    packed = rest[:quarter]
    for q in range(1, 4):
        part = pltpu.roll(rest[q * quarter : (q + 1) * quarter], 32 * q, 1)
        packed = jnp.where(lane < 32 * q, packed, part)
    return jnp.concatenate([full, packed], axis=0)


def unpack_rest(packed):
    parts = [packed] + [pltpu.roll(packed, LANES - 32 * q, 1) for q in range(1, 4)]
    return jnp.concatenate(parts, axis=0)


def widen(value):
    rows = value.shape[0]
    return jnp.concatenate([value, jnp.zeros((rows, LANES - value.shape[1]), value.dtype)], axis=1)


def pack_kernel(x_ref, out_ref):
    rhs, spheres, length = x_ref.shape
    x = x_ref[...].astype(jnp.float32).reshape(rhs * spheres, length)
    packed = pack_rows(x[:, :LANES], widen(x[:, LANES:])).astype(jnp.bfloat16)
    for d in range(out_ref.shape[0]):
        out_ref[d] = packed


def contract_kernel(
    count_ref, source_hbm, target_hbm, own_ref, odd_ref, even_ref, even_last_ref, mine_ref, other_hbm, near_out,
    source_ref, target_ref, other_ref, full_ref, rest_ref, near_ref, sems,
):
    here = lax.axis_index("gx")
    groups = lax.axis_size("gx")
    core = lax.rem(lax.axis_index("gz"), 2)
    base = pl.multiple_of((lax.axis_index("gz") - core) * mine_ref.shape[0], LANES)
    tables = []
    for i, (hbm, ref) in enumerate(((source_hbm, source_ref), (target_hbm, target_ref))):
        tables.append(pltpu.make_async_copy(hbm.at[pl.ds(base, ref.shape[0])], ref, sems.at[i]))
        tables[i].start()
    part = other_ref.shape[0] // CHUNKS
    copies = []
    for c in range(CHUNKS):
        at = pl.ds(c * part, part)
        copies.append(pltpu.make_async_copy(other_hbm.at[at], other_ref.at[at], sems.at[c + 2]))
        copies[c].start()
    slots = mine_ref.shape[0]
    spheres, rhs, _ = near_out.shape
    length = mine_ref.shape[2]
    members = own_ref.shape[0]
    rows = own_ref.shape[1] * LANES // length
    odd_block = 2 * lax.rem(here, 2)
    for ref, block in ((own_ref, 1), (odd_ref, odd_block), (even_ref, 2 - odd_block)):
        for d in range(members):
            at = pl.ds(pl.multiple_of((block * members + d) * rows, rows), rows)
            piece = ref[d].astype(jnp.float32)
            if ref is even_ref:
                piece = piece + even_last_ref[d].astype(jnp.float32)
            full_ref[at, :] = piece[:rows]
            rest_ref[at, :] = unpack_rest(piece[rows:])
    near_ref[...] = jnp.zeros_like(near_ref)
    for copy in tables:
        copy.wait()
    half = spheres // 2
    assert half & (half - 1) == 0 and groups & (groups - 1) == 0
    shift = half.bit_length() - 1
    offset = (1 - here + groups) * spheres
    live = count_ref[0] - base
    for ref, first in ((mine_ref, core * slots), (other_ref, (1 - core) * slots)):
        for p in range(slots):
            if ref is other_ref and p % part == 0:
                copies[p // part].wait()
            near_by = (source_ref[first + p] + offset) & (groups * spheres - 1)
            start = lax.shift_right_logical(near_by, shift) * (rhs * half) + (near_by & (half - 1))
            at = pl.ds(start, rhs, stride=half)
            x = jnp.concatenate([full_ref[at, :], rest_ref[at, :][:, : length - LANES]], axis=1)
            contrib = lax.dot_general(
                x.astype(jnp.bfloat16), ref[p], (((1,), (1,)), ((), ())),
                preferred_element_type=jnp.float32,
            )
            slot = jnp.where(first + p < live, target_ref[first + p], spheres)
            near_ref[slot] = near_ref[slot] + contrib
    near_out[...] = near_ref[:spheres].astype(jnp.bfloat16)


def apply_kernel(near_ref, tmat_ref, out_ref, full_ref, rest_ref):
    spheres, rhs, _ = near_ref.shape
    half = spheres // 2
    members = out_ref.shape[0]
    rows = out_ref.shape[1] * LANES // tmat_ref.shape[2]
    for s in range(spheres):
        scattered = jnp.dot(near_ref[s], tmat_ref[s], preferred_element_type=jnp.float32)
        at = pl.ds((s // half) * rhs * half + s % half, rhs, stride=half)
        full_ref[at, :] = scattered[:, :LANES]
        rest_ref[at, :] = widen(scattered[:, LANES:])
    for d in range(members):
        at = slice(d * rows, (d + 1) * rows)
        out_ref[d] = pack_rows(full_ref[at, :], rest_ref[at, :]).astype(jnp.bfloat16)


def final_kernel(x_ref, parts_ref, out_ref):
    rhs, spheres, length = x_ref.shape
    rows = rhs * spheres
    total = parts_ref[0].astype(jnp.float32)
    for d in range(1, parts_ref.shape[0]):
        total = total + parts_ref[d].astype(jnp.float32)
    rest = unpack_rest(total[rows:])[:, : length - LANES]
    scattered = jnp.concatenate([total[:rows], rest], axis=1)
    x = x_ref[...].astype(jnp.float32).reshape(rows, length)
    out_ref[...] = (x - scattered).astype(jnp.bfloat16).reshape(rhs, spheres, length)


def limit(mebibytes):
    return pltpu.CompilerParams(vmem_limit_bytes=mebibytes * 2**20)


def cost(flops, size):
    return pl.CostEstimate(flops=flops, bytes_accessed=size, transcendentals=0)


def bf16(*shape):
    return jax.ShapeDtypeStruct(shape, jnp.bfloat16)


def per_device(coeffs, translations, tmatrix, pair_target, pair_source, pair_count):
    groups = lax.axis_size("gx")
    cores = 2
    members = lax.axis_size("gy") * lax.axis_size("gz") // cores
    rhs, spheres, length = coeffs.shape
    rows = rhs * spheres
    packed = rows * length // LANES
    slots, half_length, _ = translations.shape
    group_spheres = tmatrix.shape[0]
    rhs_core = rhs * lax.axis_size("gz") // cores
    even_pairs = [(g, g ^ 1) for g in range(groups)]
    odd_pairs = [(g, (g + 1 if g % 2 else g - 1) % groups) for g in range(groups)]
    sibling = [(i, i ^ 1) for i in range(lax.axis_size("gz"))]
    same_core = [[cores * y + c for y in range(members)] for c in range(cores)]

    def exchange(pieces):
        return lax.all_to_all(
            pieces, COLUMN, split_axis=0, concat_axis=0, tiled=True, axis_index_groups=same_core
        )

    shards = pl.pallas_call(
        pack_kernel, out_shape=bf16(members, packed, LANES), in_specs=[VMEM], out_specs=VMEM,
        compiler_params=limit(2), cost_estimate=cost(10**9, 2**18), name="pack",
    )(coeffs)
    other = lax.ppermute(translations, "gz", sibling)
    own = exchange(shards)
    even_first = lax.ppermute(own, "gx", [p for p in even_pairs if p[0] % RUN < RUN - 2])
    odd = lax.ppermute(own, "gx", odd_pairs)
    even_last = lax.ppermute(own, "gx", [p for p in even_pairs if p[0] % RUN >= RUN - 2])
    window = pltpu.VMEM((3 * members * rows + spheres, LANES), jnp.float32)
    near = pl.pallas_call(
        contract_kernel,
        out_shape=bf16(group_spheres, rhs_core, half_length),
        in_specs=[SMEM] + [HBM] * 2 + [VMEM] * 5 + [HBM],
        out_specs=VMEM,
        scratch_shapes=[
            pltpu.SMEM((cores * slots,), jnp.int32),
            pltpu.SMEM((cores * slots,), jnp.int32),
            pltpu.VMEM(translations.shape, jnp.bfloat16),
            window,
            window,
            pltpu.VMEM((group_spheres + 1, rhs_core, half_length), jnp.float32),
            pltpu.SemaphoreType.DMA((CHUNKS + 2,)),
        ],
        compiler_params=limit(10),
        cost_estimate=cost(4 * rhs_core * translations.size, 4 * translations.size),
        name="contract",
    )(pair_count, pair_source, pair_target, own, odd, even_first, even_last, translations, other)
    parts = pl.pallas_call(
        apply_kernel,
        out_shape=bf16(members, packed, LANES),
        in_specs=[VMEM] * 2,
        out_specs=VMEM,
        scratch_shapes=[pltpu.VMEM((members * rows + spheres, LANES), jnp.float32)] * 2,
        compiler_params=limit(4),
        cost_estimate=cost(2 * rhs_core * tmatrix.size, 2 * tmatrix.size),
        name="apply",
    )(near, tmatrix)
    arrived = exchange(parts)
    return pl.pallas_call(
        final_kernel, out_shape=bf16(*coeffs.shape), in_specs=[VMEM] * 2, out_specs=VMEM,
        compiler_params=limit(2), name="final",
    )(coeffs, arrived)


def solution(mesh):
    placed = (
        P("gz", ("gx", "gy"), None),
        P(("gx", "gz"), "gy", None),
        P("gx", "gy", None),
        P("gx"),
        P("gx"),
        P("gx"),
    )
    return jax.shard_map(
        per_device,
        mesh=mesh,
        in_specs=placed,
        out_specs=P("gz", ("gx", "gy"), None),
        check_vma=False,
    )
```
